16 devices in a mesh: rep: 2 (over y, z), dp: 8 (over x, core).
Axes of the slice: x: 4, y: 2, z: 1, core: 2. Of those that a mesh axis runs over, the one named last changes fastest.
The devices are a block of a 4x4x8 slice.
Arguments:
- x: bfloat16 [16, 2048, 1280], P(('rep', 'dp')), parts along dimension 0
- dy: bfloat16 [16, 2048, 1280], P(('rep', 'dp')), parts along dimension 0
- w_gate: bfloat16 [2, 1280, 3584], replicated
- w_up: bfloat16 [2, 1280, 3584], replicated
- w_down: bfloat16 [2, 3584, 1280], replicated
- m_w_gate: float32 [2, 1280, 3584], P(None, 'dp')
- m_w_up: float32 [2, 1280, 3584], P(None, 'dp')
- m_w_down: float32 [2, 3584, 1280], P(None, 'dp')
- v_w_gate: float32 [2, 1280, 3584], P(None, 'dp')
- v_w_up: float32 [2, 1280, 3584], P(None, 'dp')
- v_w_down: float32 [2, 3584, 1280], P(None, 'dp')
Outputs:
- output 1: bfloat16 [4, 1280, 3584], P('rep'), parts along dimension 0
- output 2: bfloat16 [4, 1280, 3584], P('rep'), parts along dimension 0
- output 3: bfloat16 [4, 3584, 1280], P('rep'), parts along dimension 0
- output 4: float32 [4, 1280, 3584], P('rep', 'dp'), parts along dimension 0
- output 5: float32 [4, 1280, 3584], P('rep', 'dp'), parts along dimension 0
- output 6: float32 [4, 3584, 1280], P('rep', 'dp'), parts along dimension 0
- output 7: float32 [4, 1280, 3584], P('rep', 'dp'), parts along dimension 0
- output 8: float32 [4, 1280, 3584], P('rep', 'dp'), parts along dimension 0
- output 9: float32 [4, 3584, 1280], P('rep', 'dp'), parts along dimension 0
There are 2 independent parts. The reference program is written for one: setup_inputs(seed, part) draws one part's arguments, and reference() takes and returns one part's arrays. A program takes and returns all parts, laid end to end along the dimension named above; an argument that names none is the same for every part.
All inputs are finite; a program needn't handle non-finite values.
Results may differ from the reference program's by a relative error of at most 0.02.
Values are sent between devices in bfloat16 or wider.
A program may use at most 768 MiB of HBM per device.

```python
import jax
import jax.numpy as jnp
from jax import lax

SEQUENCES = 8
TOKENS = 2048
D = 1280
FF = 3584
LAYERS = 2
NAMES = ("w_gate", "w_up", "w_down")
SHAPES = {"w_gate": (LAYERS, D, FF), "w_up": (LAYERS, D, FF), "w_down": (LAYERS, FF, D)}


def bump(key, n, height):
    away = (jnp.arange(n, dtype=jnp.int32) - jax.random.randint(key, (), 0, n, jnp.int32)) % n
    return jnp.where(away < n // 8, height, 1.0)


def together(key, own, strength):
    shared = jax.random.normal(key, own.shape[1:], jnp.float32)
    return (own + strength * shared) * lax.rsqrt(1 + strength * strength)


def setup_inputs(seed: int = 0, part: int = 0) -> dict:
    kx, kdy, ka, kb, kz, kf, kh, kl, *keys = jax.random.split(jax.random.key(seed), 8 + 3 * len(NAMES))
    kx, kdy, ka, kb = (jax.random.fold_in(k, part) for k in (kx, kdy, ka, kb))
    kw, km, kv = (keys[i::3] for i in range(3))
    shape = (SEQUENCES, TOKENS, D)
    much_x, much_dy = jax.random.uniform(kz, (2,), jnp.float32, 0.0, 1.0)
    loud = 2.0 ** jax.random.uniform(jax.random.fold_in(kz, 1), (), jnp.float32, -1.0, 2.0)
    layers = 2.0 ** jax.random.uniform(kl, (LAYERS, 1, 1), jnp.float32, -1.0, 1.0)
    x = together(ka, jax.random.normal(kx, shape, jnp.float32), much_x) * bump(kf, D, 4.0)
    dy = together(kb, jax.random.normal(kdy, shape, jnp.float32), much_dy)
    drawn = {"x": x.astype(jnp.bfloat16), "dy": (loud * dy * (SEQUENCES * TOKENS) ** -0.5).astype(jnp.bfloat16)}
    for key, name in zip(kw, NAMES, strict=True):
        w = jax.random.normal(key, SHAPES[name], jnp.float32) * SHAPES[name][1] ** -0.5
        drawn[name] = (w * {"w_gate": 1.0, "w_up": bump(kh, FF, 4.0), "w_down": layers}[name]).astype(jnp.bfloat16)
    for key, name in zip(km, NAMES, strict=True):
        drawn[f"m_{name}"] = 0.1 * jax.random.normal(key, SHAPES[name], jnp.float32)
    for key, name in zip(kv, NAMES, strict=True):
        drawn[f"v_{name}"] = jax.random.uniform(key, SHAPES[name], jnp.float32, 0.005, 0.015)
    return drawn


def matmul(a, w):
    return jnp.dot(a, w, preferred_element_type=jnp.float32).astype(jnp.bfloat16)


def normed(h):
    wide = h.astype(jnp.float32)
    scale = lax.rsqrt(jnp.mean(wide**2, -1, keepdims=True) + 1e-6)
    return (wide * scale).astype(jnp.bfloat16)


def layer(h, w):
    a = normed(h)
    gate = jnp.dot(a, w["w_gate"], preferred_element_type=jnp.float32)
    up = jnp.dot(a, w["w_up"], preferred_element_type=jnp.float32)
    return h + matmul((jax.nn.silu(gate) * up).astype(jnp.bfloat16), w["w_down"])


def adamw(w, m, v, g):
    m = 0.9 * m + 0.1 * g
    v = 0.95 * v + 0.05 * g * g
    step = m * lax.rsqrt(v + 1e-8) + 0.1 * w
    return (w - 0.02 * step).astype(jnp.bfloat16), m, v


def stack(weights, h):
    return lax.scan(lambda h, w: (layer(h, w), None), h, weights)[0]


def reference(x, dy, w_gate, w_up, w_down, m_w_gate, m_w_up, m_w_down, v_w_gate, v_w_up, v_w_down):
    weights = dict(zip(NAMES, (w_gate, w_up, w_down), strict=True))

    def take(so_far, sequence):
        h, by_y = sequence
        _, back = jax.vjp(lambda w: stack(w, h), weights)
        return jax.tree.map(lambda total, term: total + term.astype(jnp.float32), so_far, back(by_y)[0]), None

    none_yet = {name: jnp.zeros(w.shape, jnp.float32) for name, w in weights.items()}
    by_weights, _ = lax.scan(take, none_yet, (x, dy))
    gradients = [by_weights[name].astype(jnp.bfloat16).astype(jnp.float32) for name in NAMES]
    new = [
        adamw(w.astype(jnp.float32), m, v, g)
        for w, m, v, g in zip((w_gate, w_up, w_down), (m_w_gate, m_w_up, m_w_down), (v_w_gate, v_w_up, v_w_down), gradients, strict=True)
    ]
    return tuple(one[which] for which in range(3) for one in new)
```

```python
import jax
import jax.numpy as jnp
from jax import lax
from jax.experimental import pallas as pl
from jax.experimental.pallas import tpu as pltpu
from jax.sharding import PartitionSpec as P

MESH = pl.DeviceIdType.MESH
STRIP = 16


def adamw(w, m, v, g):
    m = 0.9 * m + 0.1 * g
    v = 0.95 * v + 0.05 * g * g
    step = m * lax.rsqrt(v + 1e-8) + 0.1 * w
    return (w - 0.02 * step).astype(jnp.bfloat16), m, v


def strips(rows, body):
    def one(i, _):
        body(pl.ds(pl.multiple_of(i * STRIP, STRIP), STRIP))
        return ()

    lax.fori_loop(0, rows // STRIP, one, ())


class Unit:
    def __init__(self, number, place, refs, layer, cols, buf, sems):
        self.u, self.p, self.layer, self.cols, self.buf, self.sems = number, place, layer, cols, buf, sems
        self.grad, self.w, self.m, self.v, self.out, self.g = refs
        self.r = self.m.shape[1]
        self.h = self.r // 2

    def slot(self, name):
        return self.buf[name].at[self.u % self.buf[name].shape[0]]

    def sem(self, name, k=None):
        ref = self.sems[name].at[self.u % self.sems[name].shape[0]]
        return ref if k is None else ref.at[k]

    def rows(self, ref, block, half=None):
        start, size = block * self.r, self.r
        if half is not None:
            start, size = start + half * self.h, self.h
        return ref.at[pl.ds(pl.multiple_of(start, STRIP), size), self.cols]

    def remote(self, src, dst, send, recv, to):
        return pltpu.make_async_remote_copy(src_ref=src, dst_ref=dst, send_sem=send, recv_sem=recv, device_id={"dp": to}, device_id_type=MESH)

    def swap(self, k):
        p = self.p
        src = self.rows(self.grad, p.chip(k) * 2 + 1 - p.core)
        return self.remote(src, self.slot("partner").at[k], self.sem("swap_s", k), self.sem("swap_r", k), p.partner)

    def load(self, k):
        return pltpu.make_async_copy(self.rows(self.grad, self.p.chip(k) * 2 + self.p.core), self.slot("mine").at[k], self.sem("load", k))

    def first(self, side, kind):
        half = (side if kind == 0 else 1 - side) * self.h
        k = 1 if kind == 0 else (0 if side == 0 else 2)
        src = self.slot("sums").at[k, pl.ds(half, self.h)]
        i = side * 2 + kind
        return self.remote(src, self.slot("first").at[i], self.sem("first_s", i), self.sem("first_r", i), self.p.side(side))

    def second(self, side):
        src = self.slot("sums").at[0 if side == 0 else 2, pl.ds(side * self.h, self.h)]
        return self.remote(src, self.slot("second").at[side], self.sem("second_s", side), self.sem("second_r", side), self.p.side(side))

    def state(self, i):
        src = (self.m.at[self.layer, :, self.cols], self.v.at[self.layer, :, self.cols])[i] if i < 2 else self.w.at[
            self.layer, pl.ds(pl.multiple_of(self.p.me * self.r, STRIP), self.r), self.cols
        ]
        return pltpu.make_async_copy(src, self.slot(("m", "v", "w")[i]), self.sem("state", i))

    def put(self, i):
        if i == 0:
            return pltpu.make_async_copy(self.slot("new"), self.rows(self.out, self.p.me), self.sem("put", 0))
        return pltpu.make_async_copy(self.slot("g"), self.g.at[:, self.cols], self.sem("put", 1))

    def spread(self, i):
        to = self.p.partner if i == 2 else self.p.side(i)
        return self.remote(self.slot("new"), self.rows(self.out, self.p.me), self.sem("spread_s", i), self.sem("spread_r", i), to)

    def relay(self, side):
        ref = self.rows(self.out, self.p.chip(3 if side == 0 else 1) * 2 + self.p.core, side)
        return self.remote(ref, ref, self.sem("relay_s", side), self.sem("relay_r", side), self.p.side(side))

    def share(self, i):
        ref = self.rows(self.out, self.p.chip((3, 1, 2)[i]) * 2 + self.p.core)
        return self.remote(ref, ref, self.sem("share_s", i), self.sem("share_r", i), self.p.partner)

    def s0(self):
        for k in (2, 1, 3, 0):
            self.swap(k).start()
        for k in (2, 1, 3, 0):
            self.load(k).start()

    def s1(self):
        mine, partner, sums = self.slot("mine"), self.slot("partner"), self.slot("sums")
        for k in (2, 1, 3):
            self.load(k).wait()
            self.swap(k).wait_recv()

            def add(rows, k=k):
                sums[k - 1, rows] = (mine[k, rows].astype(jnp.float32) + partner[k, rows].astype(jnp.float32)).astype(jnp.bfloat16)

            strips(self.r, add)
            if k == 2:
                for side in range(2):
                    self.first(side, 0).start()
            else:
                self.first(0 if k == 1 else 1, 1).start()
        for i in range(3):
            self.state(i).start()

    def s2(self):
        sums, first = self.slot("sums"), self.slot("first")
        for side in range(2):
            self.first(side, 0).wait_recv()
            k, start = 0 if side == 0 else 2, side * self.h

            def add(i, _, side=side, k=k, start=start):
                here = pl.ds(pl.multiple_of(start + i * STRIP, STRIP), STRIP)
                there = pl.ds(pl.multiple_of(i * STRIP, STRIP), STRIP)
                sums[k, here] = (sums[k, here].astype(jnp.float32) + first[side * 2, there].astype(jnp.float32)).astype(jnp.bfloat16)
                return ()

            lax.fori_loop(0, self.h // STRIP, add, ())
            self.second(side).start()

    def s3(self):
        mine, partner, first, second = (self.slot(name) for name in ("mine", "partner", "first", "second"))
        m, v, w, g, new = (self.slot(name) for name in ("m", "v", "w", "g", "new"))
        self.load(0).wait()
        self.swap(0).wait_recv()
        for i in range(3):
            self.state(i).wait()
        for side in range(2):
            self.first(side, 1).wait_recv()
            self.second(side).wait_recv()
        for side in range(2):
            def step(i, _, side=side):
                here = pl.ds(pl.multiple_of(side * self.h + i * STRIP, STRIP), STRIP)
                there = pl.ds(pl.multiple_of(i * STRIP, STRIP), STRIP)
                total = mine[0, here].astype(jnp.float32) + partner[0, here].astype(jnp.float32)
                total = total + second[side, there].astype(jnp.float32) + first[(1 - side) * 2 + 1, there].astype(jnp.float32)
                rounded = total.astype(jnp.bfloat16)
                g[here] = rounded
                new[here] = adamw(w[here].astype(jnp.float32), m[here], v[here], rounded.astype(jnp.float32))[0]
                return ()

            lax.fori_loop(0, self.h // STRIP, step, ())
        for i in range(3):
            self.spread(i).start()
        for i in range(2):
            self.put(i).start()
        for k in range(4):
            self.swap(k).wait_send()
        for i in range(4):
            self.first(i // 2, i % 2).wait_send()
        for side in range(2):
            self.second(side).wait_send()

    def s4(self):
        for side in range(2):
            self.spread(side).wait_recv()
            self.relay(side).start()
            self.share(side).start()
        self.spread(2).wait_recv()
        for i in range(3):
            self.spread(i).wait_send()
        for i in range(2):
            self.put(i).wait()

    def s5(self):
        for side in range(2):
            self.relay(side).wait_recv()
        self.share(2).start()
        for side in range(2):
            self.relay(side).wait_send()
            self.share(side).wait()

    def s6(self):
        self.share(2).wait()


class Place:
    def __init__(self, size):
        assert size == 8
        self.me = lax.axis_index("dp")
        self.core = lax.rem(self.me, 2)
        self.at = self.me // 2
        self.partner = self.me + 1 - 2 * self.core

    def chip(self, k):
        return lax.rem(self.at + k, 4)

    def side(self, side):
        return self.chip(1 if side == 0 else 3) * 2 + self.core


RING = {"mine": 4, "partner": 4, "sums": 3, "first": 3, "second": 3, "m": 3, "v": 3, "w": 3, "g": 3, "new": 3}
SEMS = {"swap_s": 4, "swap_r": 4, "load": 4, "first_s": 4, "first_r": 4, "second_s": 2, "second_r": 2, "state": 3, "put": 2,
        "spread_s": 3, "spread_r": 3, "relay_s": 2, "relay_r": 2, "share_s": 3, "share_r": 3}
DEEP = 7


def buffers(r, c):
    h = r // 2
    shapes = {"mine": (4, r, c), "partner": (4, r, c), "sums": (3, r, c), "first": (4, h, c), "second": (2, h, c)}
    shapes.update({name: (r, c) for name in ("m", "v", "w", "g", "new")})
    return {name: pltpu.VMEM((RING[name], *shape), jnp.float32 if name in ("m", "v") else jnp.bfloat16) for name, shape in shapes.items()}


def widths(r, columns):
    target = 150_000 // r
    best = 128
    for c in range(128, columns + 1, 128):
        if columns % c == 0 and abs(c - target) < abs(best - target):
            best = c
    return best


def fit(n, *sizes):
    return next(s for s in sizes if n % s == 0)


def contract(a, b, dims):
    return lax.dot_general(a, b, ((dims, dims), ((), ())), preferred_element_type=jnp.float32)


def gradient_piece(a, b, out):
    tokens, rows = a.shape
    columns = b.shape[1]

    def body(a, b, out):
        out[...] = contract(a[...], b[...], (0,)).astype(jnp.bfloat16)

    if rows <= columns:
        tm, tn = rows, fit(columns, 256, 128)
    else:
        tm, tn = fit(rows, 512, 256, 128), columns
    pltpu.emit_pipeline(
        body,
        grid=(rows // tm, columns // tn),
        in_specs=[pl.BlockSpec((tokens, tm), lambda i, j: (0, i)), pl.BlockSpec((tokens, tn), lambda i, j: (0, j))],
        out_specs=[pl.BlockSpec((tm, tn), lambda i, j: (i, j))],
    )(a, b, out)


def hidden_piece(dy, w, gate, up, dgate, dup):
    tokens, d = dy.shape
    ff = w.shape[0]
    tn = fit(ff, 256, 128)

    def body(dy, w, gate, up, dgate, dup):
        dp = contract(dy[...], w[...], (1,)).astype(jnp.bfloat16).astype(jnp.float32)
        dgate[...] = (dp * gate[...]).astype(jnp.bfloat16)
        dup[...] = (dp * up[...]).astype(jnp.bfloat16)

    tile = pl.BlockSpec((tokens, tn), lambda j: (0, j))
    pltpu.emit_pipeline(
        body,
        grid=(ff // tn,),
        in_specs=[pl.BlockSpec((tokens, d), lambda j: (0, 0)), pl.BlockSpec((tn, d), lambda j: (j, 0)), tile, tile],
        out_specs=[tile, tile],
    )(dy, w, gate, up, dgate, dup)


def input_piece(dh, w, out, other=None):
    tokens, ff = dh.shape
    columns = w.shape[0]
    tn = fit(columns, 256, 128)

    def body(dh, w, *rest):
        new = contract(dh[...], w[...], (1,)).astype(jnp.bfloat16)
        rest[-1][...] = rest[0][...] + new if len(rest) > 1 else new

    tile = pl.BlockSpec((tokens, tn), lambda j: (0, j))
    pltpu.emit_pipeline(
        body,
        grid=(columns // tn,),
        in_specs=[pl.BlockSpec((tokens, ff), lambda j: (0, 0)), pl.BlockSpec((tn, ff), lambda j: (j, 0))] + [tile] * (other is not None),
        out_specs=[tile],
    )(dh, w, *([] if other is None else [other]), out)


def norm_piece(h, da, dy, out):
    tokens, d = h.shape
    tm = fit(tokens, 256, 128)

    def body(h, da, dy, out):
        wide, da = h[...].astype(jnp.float32), da[...].astype(jnp.float32)
        scale = lax.rsqrt(jnp.mean(wide**2, -1, keepdims=True) + 1e-6)
        back = da * scale - wide * (scale * scale * scale * jnp.mean(da * wide, -1, keepdims=True))
        out[...] = dy[...] + back.astype(jnp.bfloat16)

    tile = pl.BlockSpec((tm, d), lambda i: (i, 0))
    pltpu.emit_pipeline(body, grid=(tokens // tm,), in_specs=[tile] * 3, out_specs=[tile])(h, da, dy, out)


BUDGET = 20.0


def backward(size, number, n, layers, above, saved, below, given, ws, ms, vs):
    d, ff = ws[0].shape[1:]
    tokens = above.shape[0]
    shapes = [w.shape[1:] for w in ws]
    kinds = sorted(set(shapes))
    width = {k: widths(k[0] // size, k[1]) for k in kinds}
    bf = jnp.bfloat16
    like = jax.ShapeDtypeStruct
    groups = [("above", [above]), ("w", ws), ("m", ms), ("v", vs)] + [(name, [saved[name]]) for name in ("a", "h", "slope", "silu", "p")]
    results = [("new", [like(s, bf) for s in shapes]), ("block", [like((s[0] // size, s[1]), bf) for s in shapes])]
    results += [("grad", [like(s, bf) for s in shapes[:2]])]
    if given is None:
        results += [("given", [like(shapes[2], bf)] + [like((tokens, ff), bf)] * 2)]
    else:
        groups += [("given", given)]
    if below is not None:
        groups += [("b_" + name, [below[name]]) for name in ("slope", "silu", "p")]
        results += [("next", [like(shapes[2], bf)] + [like((tokens, ff), bf)] * 2)]
        results += [(name, [like((tokens, d), bf)]) for name in ("part", "da", "dh")]

    def kernel(*refs):
        at = 0
        ref = {}
        for name, arrays in groups + results:
            ref[name] = refs[at : at + len(arrays)]
            at += len(arrays)
        bufs = {}
        for k in kinds:
            bufs[k] = dict(zip(RING, refs[at : at + len(RING)], strict=True))
            at += len(RING)
        sems = dict(zip(SEMS, refs[at:], strict=True))
        place = Place(size)
        barrier = pltpu.get_barrier_semaphore()
        for to in (place.partner, place.side(0), place.side(1)):
            pl.semaphore_signal(barrier, inc=1, device_id={"dp": to}, device_id_type=MESH)
        pl.semaphore_wait(barrier, 3)

        units, pieces, ready = [], [], []

        def weight(which, grad, a=None, b=None, send=True):
            shape = shapes[which]
            c = width[shape]
            count = shape[1] // c
            for first, last in ((0, (count + 1) // 2), ((count + 1) // 2, count)):
                some = pl.ds(first * c, (last - first) * c)
                if a is not None:
                    cost = 2 * tokens * shape[0] * c * (last - first) / 0.8e9 + 2
                    pieces.append((cost, lambda some=some: gradient_piece(a, b.at[:, some], grad.at[:, some])))
                for i in range(first, last) if send else ():
                    the = (grad, *(ref[x][which] for x in ("w", "m", "v", "new", "block")))
                    units.append(Unit(len(units), place, the, n, pl.ds(i * c, c), bufs[shape], sems))
                    ready.append(len(pieces))

        def hidden(n, above, slope, silu, dgate, dup):
            for start in range(0, tokens, tokens // 2):
                some = pl.ds(start, tokens // 2)
                pieces.append((20, lambda some=some: hidden_piece(
                    above.at[some], ref["w"][2].at[n], *(one.at[some] for one in (slope, silu, dgate, dup)))))

        above, (a,), (h,) = ref["above"][0], ref["a"], ref["h"]
        down, dgate, dup = ref["given"]
        if given is None:
            weight(2, down, ref["p"][0], above)
            hidden(n, above, ref["slope"][0], ref["silu"][0], dgate, dup)
        else:
            weight(2, down)
        weight(0, ref["grad"][0], a, dgate)
        weight(1, ref["grad"][1], a, dup)
        if below is not None:
            (part,), (da,), (dh,) = ref["part"], ref["da"], ref["dh"]
            for start in range(0, tokens, tokens // 2):
                some = pl.ds(start, tokens // 2)
                pieces.append((17, lambda some=some: input_piece(dgate.at[some], ref["w"][0].at[n], part.at[some])))
                pieces.append((17, lambda some=some: input_piece(dup.at[some], ref["w"][1].at[n], da.at[some], part.at[some])))
            pieces.append((9, lambda: norm_piece(h, da, above, dh)))
            weight(2, ref["next"][0], ref["b_p"][0], dh, send=False)
            hidden(n - 1, dh, ref["b_slope"][0], ref["b_silu"][0], *ref["next"][1:])

        done = 0
        for t in range(len(units) + 6):
            if t < len(units):
                while done < ready[t]:
                    pieces[done][1]()
                    done += 1
            for stage in range(6, -1, -1):
                if 0 <= t - stage < len(units):
                    getattr(units[t - stage], f"s{stage}")()
            spent = 0.0
            while done < len(pieces) and spent + pieces[done][0] <= BUDGET:
                spent += pieces[done][0]
                pieces[done][1]()
                done += 1
        while done < len(pieces):
            pieces[done][1]()
            done += 1

    anywhere = pl.BlockSpec(memory_space=pl.ANY)
    scratch = []
    for k in kinds:
        scratch += list(buffers(k[0] // size, width[k]).values())
    scratch += [pltpu.SemaphoreType.DMA((DEEP, count)) for count in SEMS.values()]
    operands = [one for _, arrays in groups for one in arrays]
    outs = [one for _, arrays in results for one in arrays]
    out = pl.pallas_call(
        kernel,
        out_shape=outs,
        in_specs=[anywhere] * len(operands),
        out_specs=[anywhere] * len(outs),
        scratch_shapes=scratch,
        compiler_params=pltpu.CompilerParams(collective_id=number, has_side_effects=True, vmem_limit_bytes=63 * 2**20),
        name=f"backward{number}",
    )(*operands)
    got, at = {}, 0
    for name, arrays in results:
        got[name] = list(out[at : at + len(arrays)])
        at += len(arrays)
    return got


def matmul(a, w):
    return jnp.dot(a, w, preferred_element_type=jnp.float32).astype(jnp.bfloat16)


def normed(h):
    wide = h.astype(jnp.float32)
    scale = lax.rsqrt(jnp.mean(wide**2, -1, keepdims=True) + 1e-6)
    return (wide * scale).astype(jnp.bfloat16)


def solution(mesh):
    size = mesh.shape["dp"]

    def local(x, dy, *arrays):
        ws, ms, vs = (arrays[i : i + 3] for i in (0, 3, 6))
        h, dy = x[0], dy[0]
        layers = ws[0].shape[0]
        saved = []
        for n in range(layers):
            a = normed(h)
            gate = jnp.dot(a, ws[0][n], preferred_element_type=jnp.float32)
            up = jnp.dot(a, ws[1][n], preferred_element_type=jnp.float32)
            share = jax.nn.sigmoid(gate)
            silu = gate * share
            p = (silu * up).astype(jnp.bfloat16)
            slope = up * (share + silu * (1 - share))
            saved.append({"a": a, "h": h, "slope": slope, "silu": silu, "p": p})
            if n < layers - 1:
                h = h + matmul(p, ws[2][n])
        new, blocks, given = [None] * layers, [None] * layers, None
        for number, n in enumerate(reversed(range(layers))):
            got = backward(size, number, n, layers, dy, saved[n], saved[n - 1] if n else None, given, ws, ms, vs)
            new[n], blocks[n] = got["new"], got["block"]
            if n:
                given, dy = got["next"], got["dh"][0]
        new, blocks = ([jnp.stack(one) for one in zip(*all, strict=True)] for all in (new, blocks))
        out_m, out_v = [], []
        for g, m, v in zip(blocks, ms, vs, strict=True):
            g = g.astype(jnp.float32)
            _, m, v = adamw(jnp.zeros_like(g), m, v, g)
            out_m.append(m)
            out_v.append(v)
        return (*new, *out_m, *out_v)

    tokens, whole, rows, groups = P(("rep", "dp"), None, None), P(None, None, None), P(None, "dp", None), P("rep", None, None)
    return jax.shard_map(
        local,
        mesh=mesh,
        in_specs=(tokens,) * 2 + (whole,) * 3 + (rows,) * 6,
        out_specs=(groups,) * 3 + (P("rep", "dp", None),) * 6,
        check_vma=False,
    )
```

```python
import jax
import jax.numpy as jnp
from jax import lax
from jax.experimental import pallas as pl
from jax.experimental.pallas import tpu as pltpu
from jax.sharding import PartitionSpec as P

MESH = pl.DeviceIdType.MESH
STRIP = 16


def adamw(w, m, v, g):
    m = 0.9 * m + 0.1 * g
    v = 0.95 * v + 0.05 * g * g
    step = m * lax.rsqrt(v + 1e-8) + 0.1 * w
    return (w - 0.02 * step).astype(jnp.bfloat16), m, v


def strips(rows, body):
    def one(i, _):
        body(pl.ds(pl.multiple_of(i * STRIP, STRIP), STRIP))
        return ()

    lax.fori_loop(0, rows // STRIP, one, ())


class Unit:
    def __init__(self, number, place, refs, layer, cols, buf, sems):
        self.u, self.p, self.layer, self.cols, self.buf, self.sems = number, place, layer, cols, buf, sems
        self.grad, self.w, self.m, self.v, self.out, self.g = refs
        self.r = self.m.shape[1]
        self.h = self.r // 2

    def slot(self, name):
        return self.buf[name].at[self.u % self.buf[name].shape[0]]

    def sem(self, name, k=None):
        ref = self.sems[name].at[self.u % self.sems[name].shape[0]]
        return ref if k is None else ref.at[k]

    def rows(self, ref, block, half=None):
        start, size = block * self.r, self.r
        if half is not None:
            start, size = start + half * self.h, self.h
        return ref.at[pl.ds(pl.multiple_of(start, STRIP), size), self.cols]

    def remote(self, src, dst, send, recv, to):
        return pltpu.make_async_remote_copy(src_ref=src, dst_ref=dst, send_sem=send, recv_sem=recv, device_id={"dp": to}, device_id_type=MESH)

    def swap(self, k):
        p = self.p
        src = self.rows(self.grad, p.chip(k) * 2 + 1 - p.core)
        return self.remote(src, self.slot("partner").at[k], self.sem("swap_s", k), self.sem("swap_r", k), p.partner)

    def load(self, k):
        return pltpu.make_async_copy(self.rows(self.grad, self.p.chip(k) * 2 + self.p.core), self.slot("mine").at[k], self.sem("load", k))

    def first(self, side, kind):
        half = (side if kind == 0 else 1 - side) * self.h
        k = 1 if kind == 0 else (0 if side == 0 else 2)
        src = self.slot("sums").at[k, pl.ds(half, self.h)]
        i = side * 2 + kind
        return self.remote(src, self.slot("first").at[i], self.sem("first_s", i), self.sem("first_r", i), self.p.side(side))

    def second(self, side):
        src = self.slot("sums").at[0 if side == 0 else 2, pl.ds(side * self.h, self.h)]
        return self.remote(src, self.slot("second").at[side], self.sem("second_s", side), self.sem("second_r", side), self.p.side(side))

    def state(self, i):
        src = (self.m.at[self.layer, :, self.cols], self.v.at[self.layer, :, self.cols])[i] if i < 2 else self.w.at[
            self.layer, pl.ds(pl.multiple_of(self.p.me * self.r, STRIP), self.r), self.cols
        ]
        return pltpu.make_async_copy(src, self.slot(("m", "v", "w")[i]), self.sem("state", i))

    def put(self, i):
        if i == 0:
            return pltpu.make_async_copy(self.slot("new"), self.rows(self.out, self.p.me), self.sem("put", 0))
        return pltpu.make_async_copy(self.slot("g"), self.g.at[:, self.cols], self.sem("put", 1))

    def spread(self, i):
        to = self.p.partner if i == 2 else self.p.side(i)
        return self.remote(self.slot("new"), self.rows(self.out, self.p.me), self.sem("spread_s", i), self.sem("spread_r", i), to)

    def relay(self, side):
        ref = self.rows(self.out, self.p.chip(3 if side == 0 else 1) * 2 + self.p.core, side)
        return self.remote(ref, ref, self.sem("relay_s", side), self.sem("relay_r", side), self.p.side(side))

    def share(self, i):
        ref = self.rows(self.out, self.p.chip((3, 1, 2)[i]) * 2 + self.p.core)
        return self.remote(ref, ref, self.sem("share_s", i), self.sem("share_r", i), self.p.partner)

    def s0(self):
        for k in (2, 1, 3, 0):
            self.swap(k).start()
        for k in (2, 1, 3, 0):
            self.load(k).start()

    def s1(self):
        mine, partner, sums = self.slot("mine"), self.slot("partner"), self.slot("sums")
        for k in (2, 1, 3):
            self.load(k).wait()
            self.swap(k).wait_recv()

            def add(rows, k=k):
                sums[k - 1, rows] = (mine[k, rows].astype(jnp.float32) + partner[k, rows].astype(jnp.float32)).astype(jnp.bfloat16)

            strips(self.r, add)
            if k == 2:
                for side in range(2):
                    self.first(side, 0).start()
            else:
                self.first(0 if k == 1 else 1, 1).start()
        for i in range(3):
            self.state(i).start()

    def s2(self):
        sums, first = self.slot("sums"), self.slot("first")
        for side in range(2):
            self.first(side, 0).wait_recv()
            k, start = 0 if side == 0 else 2, side * self.h

            def add(i, _, side=side, k=k, start=start):
                here = pl.ds(pl.multiple_of(start + i * STRIP, STRIP), STRIP)
                there = pl.ds(pl.multiple_of(i * STRIP, STRIP), STRIP)
                sums[k, here] = (sums[k, here].astype(jnp.float32) + first[side * 2, there].astype(jnp.float32)).astype(jnp.bfloat16)
                return ()

            lax.fori_loop(0, self.h // STRIP, add, ())
            self.second(side).start()

    def s3(self):
        mine, partner, first, second = (self.slot(name) for name in ("mine", "partner", "first", "second"))
        m, v, w, g, new = (self.slot(name) for name in ("m", "v", "w", "g", "new"))
        self.load(0).wait()
        self.swap(0).wait_recv()
        for i in range(3):
            self.state(i).wait()
        for side in range(2):
            self.first(side, 1).wait_recv()
            self.second(side).wait_recv()
        for side in range(2):
            def step(i, _, side=side):
                here = pl.ds(pl.multiple_of(side * self.h + i * STRIP, STRIP), STRIP)
                there = pl.ds(pl.multiple_of(i * STRIP, STRIP), STRIP)
                total = mine[0, here].astype(jnp.float32) + partner[0, here].astype(jnp.float32)
                total = total + second[side, there].astype(jnp.float32) + first[(1 - side) * 2 + 1, there].astype(jnp.float32)
                rounded = total.astype(jnp.bfloat16)
                g[here] = rounded
                new[here] = adamw(w[here].astype(jnp.float32), m[here], v[here], rounded.astype(jnp.float32))[0]
                return ()

            lax.fori_loop(0, self.h // STRIP, step, ())
        for i in range(3):
            self.spread(i).start()
        for i in range(2):
            self.put(i).start()
        for k in range(4):
            self.swap(k).wait_send()
        for i in range(4):
            self.first(i // 2, i % 2).wait_send()
        for side in range(2):
            self.second(side).wait_send()

    def s4(self):
        for side in range(2):
            self.spread(side).wait_recv()
            self.relay(side).start()
            self.share(side).start()
        self.spread(2).wait_recv()
        for i in range(3):
            self.spread(i).wait_send()
        for i in range(2):
            self.put(i).wait()

    def s5(self):
        for side in range(2):
            self.relay(side).wait_recv()
        self.share(2).start()
        for side in range(2):
            self.relay(side).wait_send()
            self.share(side).wait()

    def s6(self):
        self.share(2).wait()


class Place:
    def __init__(self, size):
        assert size == 8
        self.me = lax.axis_index("dp")
        self.core = lax.rem(self.me, 2)
        self.at = self.me // 2
        self.partner = self.me + 1 - 2 * self.core

    def chip(self, k):
        return lax.rem(self.at + k, 4)

    def side(self, side):
        return self.chip(1 if side == 0 else 3) * 2 + self.core


RING = {"mine": 4, "partner": 4, "sums": 3, "first": 3, "second": 3, "m": 3, "v": 3, "w": 3, "g": 3, "new": 3}
SEMS = {"swap_s": 4, "swap_r": 4, "load": 4, "first_s": 4, "first_r": 4, "second_s": 2, "second_r": 2, "state": 3, "put": 2,
        "spread_s": 3, "spread_r": 3, "relay_s": 2, "relay_r": 2, "share_s": 3, "share_r": 3}
DEEP = 7


def buffers(r, c):
    h = r // 2
    shapes = {"mine": (4, r, c), "partner": (4, r, c), "sums": (3, r, c), "first": (4, h, c), "second": (2, h, c)}
    shapes.update({name: (r, c) for name in ("m", "v", "w", "g", "new")})
    return {name: pltpu.VMEM((RING[name], *shape), jnp.float32 if name in ("m", "v") else jnp.bfloat16) for name, shape in shapes.items()}


def widths(r, columns):
    target = 150_000 // r
    best = 128
    for c in range(128, columns + 1, 128):
        if columns % c == 0 and abs(c - target) < abs(best - target):
            best = c
    return best


def fit(n, *sizes):
    return next(s for s in sizes if n % s == 0)


def contract(a, b, dims):
    return lax.dot_general(a, b, ((dims, dims), ((), ())), preferred_element_type=jnp.float32)


def gradient_piece(a, b, out):
    tokens, rows = a.shape
    columns = b.shape[1]

    def body(a, b, out):
        out[...] = contract(a[...], b[...], (0,)).astype(jnp.bfloat16)

    if rows <= columns:
        tm, tn = rows, fit(columns, 256, 128)
    else:
        tm, tn = fit(rows, 512, 256, 128), columns
    pltpu.emit_pipeline(
        body,
        grid=(rows // tm, columns // tn),
        in_specs=[pl.BlockSpec((tokens, tm), lambda i, j: (0, i)), pl.BlockSpec((tokens, tn), lambda i, j: (0, j))],
        out_specs=[pl.BlockSpec((tm, tn), lambda i, j: (i, j))],
    )(a, b, out)


def hidden_piece(dy, w, gate, up, dgate, dup):
    tokens, d = dy.shape
    ff = w.shape[0]
    tn = fit(ff, 256, 128)

    def body(dy, w, gate, up, dgate, dup):
        dp = contract(dy[...], w[...], (1,)).astype(jnp.bfloat16).astype(jnp.float32)
        dgate[...] = (dp * gate[...]).astype(jnp.bfloat16)
        dup[...] = (dp * up[...]).astype(jnp.bfloat16)

    tile = pl.BlockSpec((tokens, tn), lambda j: (0, j))
    pltpu.emit_pipeline(
        body,
        grid=(ff // tn,),
        in_specs=[pl.BlockSpec((tokens, d), lambda j: (0, 0)), pl.BlockSpec((tn, d), lambda j: (j, 0)), tile, tile],
        out_specs=[tile, tile],
    )(dy, w, gate, up, dgate, dup)


def input_piece(dh, w, out, other=None):
    tokens, ff = dh.shape
    columns = w.shape[0]
    tn = fit(columns, 256, 128)

    def body(dh, w, *rest):
        new = contract(dh[...], w[...], (1,)).astype(jnp.bfloat16)
        rest[-1][...] = rest[0][...] + new if len(rest) > 1 else new

    tile = pl.BlockSpec((tokens, tn), lambda j: (0, j))
    pltpu.emit_pipeline(
        body,
        grid=(columns // tn,),
        in_specs=[pl.BlockSpec((tokens, ff), lambda j: (0, 0)), pl.BlockSpec((tn, ff), lambda j: (j, 0))] + [tile] * (other is not None),
        out_specs=[tile],
    )(dh, w, *([] if other is None else [other]), out)


def norm_piece(h, da, dy, out):
    tokens, d = h.shape
    tm = fit(tokens, 256, 128)

    def body(h, da, dy, out):
        wide, da = h[...].astype(jnp.float32), da[...].astype(jnp.float32)
        scale = lax.rsqrt(jnp.mean(wide**2, -1, keepdims=True) + 1e-6)
        back = da * scale - wide * (scale * scale * scale * jnp.mean(da * wide, -1, keepdims=True))
        out[...] = dy[...] + back.astype(jnp.bfloat16)

    tile = pl.BlockSpec((tm, d), lambda i: (i, 0))
    pltpu.emit_pipeline(body, grid=(tokens // tm,), in_specs=[tile] * 3, out_specs=[tile])(h, da, dy, out)


BUDGET = 20.0


def backward(size, number, n, layers, above, saved, below, given, ws, ms, vs):
    d, ff = ws[0].shape[1:]
    tokens = above.shape[0]
    shapes = [w.shape[1:] for w in ws]
    kinds = sorted(set(shapes))
    width = {k: widths(k[0] // size, k[1]) for k in kinds}
    bf = jnp.bfloat16
    like = jax.ShapeDtypeStruct
    groups = [("above", [above]), ("w", ws), ("m", ms), ("v", vs)] + [(name, [saved[name]]) for name in ("a", "h", "slope", "silu", "p")]
    results = [("new", [like(s, bf) for s in shapes]), ("block", [like((s[0] // size, s[1]), bf) for s in shapes])]
    results += [("grad", [like(s, bf) for s in shapes[:2]])]
    if given is None:
        results += [("given", [like(shapes[2], bf)] + [like((tokens, ff), bf)] * 2)]
    else:
        groups += [("given", given)]
        results += [("hidden", [like((tokens, ff), bf)] * 2)]
    if below is not None:
        groups += [("b_p", [below["p"]])]
        results += [("next", [like(shapes[2], bf)])]
        results += [(name, [like((tokens, d), bf)]) for name in ("part", "da", "dh")]

    def kernel(*refs):
        at = 0
        ref = {}
        for name, arrays in groups + results:
            ref[name] = refs[at : at + len(arrays)]
            at += len(arrays)
        bufs = {}
        for k in kinds:
            bufs[k] = dict(zip(RING, refs[at : at + len(RING)], strict=True))
            at += len(RING)
        sems = dict(zip(SEMS, refs[at:], strict=True))
        place = Place(size)
        barrier = pltpu.get_barrier_semaphore()
        for to in (place.partner, place.side(0), place.side(1)):
            pl.semaphore_signal(barrier, inc=1, device_id={"dp": to}, device_id_type=MESH)
        pl.semaphore_wait(barrier, 3)

        units, pieces, ready = [], [], []

        def weight(which, grad, a=None, b=None, send=True):
            shape = shapes[which]
            c = width[shape]
            count = shape[1] // c
            for first, last in ((0, (count + 1) // 2), ((count + 1) // 2, count)):
                some = pl.ds(first * c, (last - first) * c)
                if a is not None:
                    cost = 2 * tokens * shape[0] * c * (last - first) / 0.8e9 + 2
                    pieces.append((cost, lambda some=some: gradient_piece(a, b.at[:, some], grad.at[:, some])))
                for i in range(first, last) if send else ():
                    the = (grad, *(ref[x][which] for x in ("w", "m", "v", "new", "block")))
                    units.append(Unit(len(units), place, the, n, pl.ds(i * c, c), bufs[shape], sems))
                    ready.append(len(pieces))

        def hidden(n, above, slope, silu, dgate, dup):
            for start in range(0, tokens, tokens // 2):
                some = pl.ds(start, tokens // 2)
                pieces.append((20, lambda some=some: hidden_piece(
                    above.at[some], ref["w"][2].at[n], *(one.at[some] for one in (slope, silu, dgate, dup)))))

        above, (a,), (h,) = ref["above"][0], ref["a"], ref["h"]
        if given is None:
            down, dgate, dup = ref["given"]
            weight(2, down, ref["p"][0], above)
        else:
            (down,), (dgate, dup) = ref["given"], ref["hidden"]
            weight(2, down)
        hidden(n, above, ref["slope"][0], ref["silu"][0], dgate, dup)
        weight(0, ref["grad"][0], a, dgate)
        weight(1, ref["grad"][1], a, dup)
        if below is not None:
            (part,), (da,), (dh,) = ref["part"], ref["da"], ref["dh"]
            for start in range(0, tokens, tokens // 2):
                some = pl.ds(start, tokens // 2)
                pieces.append((17, lambda some=some: input_piece(dgate.at[some], ref["w"][0].at[n], part.at[some])))
                pieces.append((17, lambda some=some: input_piece(dup.at[some], ref["w"][1].at[n], da.at[some], part.at[some])))
            pieces.append((9, lambda: norm_piece(h, da, above, dh)))
            weight(2, ref["next"][0], ref["b_p"][0], dh, send=False)

        done = 0
        for t in range(len(units) + 6):
            if t < len(units):
                while done < ready[t]:
                    pieces[done][1]()
                    done += 1
            for stage in range(6, -1, -1):
                if 0 <= t - stage < len(units):
                    getattr(units[t - stage], f"s{stage}")()
            spent = 0.0
            while done < len(pieces) and spent + pieces[done][0] <= BUDGET:
                spent += pieces[done][0]
                pieces[done][1]()
                done += 1
        while done < len(pieces):
            pieces[done][1]()
            done += 1

    anywhere = pl.BlockSpec(memory_space=pl.ANY)
    scratch = []
    for k in kinds:
        scratch += list(buffers(k[0] // size, width[k]).values())
    scratch += [pltpu.SemaphoreType.DMA((DEEP, count)) for count in SEMS.values()]
    operands = [one for _, arrays in groups for one in arrays]
    outs = [one for _, arrays in results for one in arrays]
    out = pl.pallas_call(
        kernel,
        out_shape=outs,
        in_specs=[anywhere] * len(operands),
        out_specs=[anywhere] * len(outs),
        scratch_shapes=scratch,
        compiler_params=pltpu.CompilerParams(collective_id=number, has_side_effects=True, vmem_limit_bytes=63 * 2**20),
        name=f"backward{number}",
    )(*operands)
    got, at = {}, 0
    for name, arrays in results:
        got[name] = list(out[at : at + len(arrays)])
        at += len(arrays)
    return got


def matmul(a, w):
    return jnp.dot(a, w, preferred_element_type=jnp.float32).astype(jnp.bfloat16)


def normed(h):
    wide = h.astype(jnp.float32)
    scale = lax.rsqrt(jnp.mean(wide**2, -1, keepdims=True) + 1e-6)
    return (wide * scale).astype(jnp.bfloat16)


def solution(mesh):
    size = mesh.shape["dp"]

    def local(x, dy, *arrays):
        ws, ms, vs = (arrays[i : i + 3] for i in (0, 3, 6))
        h, dy = x[0], dy[0]
        layers = ws[0].shape[0]
        saved = []
        for n in range(layers):
            a = normed(h)
            gate = jnp.dot(a, ws[0][n], preferred_element_type=jnp.float32)
            up = jnp.dot(a, ws[1][n], preferred_element_type=jnp.float32)
            share = jax.nn.sigmoid(gate)
            silu = gate * share
            p = (silu * up).astype(jnp.bfloat16)
            slope = up * (share + silu * (1 - share))
            saved.append({"a": a, "h": h, "slope": slope, "silu": silu, "p": p})
            if n < layers - 1:
                h = h + matmul(p, ws[2][n])
        new, blocks, given = [None] * layers, [None] * layers, None
        for number, n in enumerate(reversed(range(layers))):
            got = backward(size, number, n, layers, dy, saved[n], saved[n - 1] if n else None, given, ws, ms, vs)
            new[n], blocks[n] = got["new"], got["block"]
            if n:
                given, dy = got["next"], got["dh"][0]
        new, blocks = ([jnp.stack(one) for one in zip(*all, strict=True)] for all in (new, blocks))
        out_m, out_v = [], []
        for g, m, v in zip(blocks, ms, vs, strict=True):
            g = g.astype(jnp.float32)
            _, m, v = adamw(jnp.zeros_like(g), m, v, g)
            out_m.append(m)
            out_v.append(v)
        return (*new, *out_m, *out_v)

    tokens, whole, rows, groups = P(("rep", "dp"), None, None), P(None, None, None), P(None, "dp", None), P("rep", None, None)
    return jax.shard_map(
        local,
        mesh=mesh,
        in_specs=(tokens,) * 2 + (whole,) * 3 + (rows,) * 6,
        out_specs=(groups,) * 3 + (P("rep", "dp", None),) * 6,
        check_vma=False,
    )
```
